256 devices in a mesh: krow: 32 (over z, x_lo, core), kcol: 8 (over x_hi, y).
Axes of the slice: x: 4 (x_hi: 2, x_lo: 2; x = x_hi * 2 + x_lo), y: 4, z: 8, core: 2. Of those that a mesh axis runs over, the one named last changes fastest.
Arguments:
- green: bfloat16 [4, 2, 32, 16, 256, 256], P(None, None, 'krow', 'kcol'), may hold values from -6 to 6
- screened: float32 [32, 16, 65536], P(None, None, ('krow', 'kcol')), may hold values from 0.1 to 1
Outputs:
- sigma: bfloat16 [4, 2, 32, 16, 256, 256], P(None, None, 'krow', 'kcol')
- dressed: bfloat16 [4, 2, 32, 16, 256, 256], P(None, None, 'krow', 'kcol')
The draws below stay inside these ranges and needn't reach their ends.
All inputs are finite; a program needn't handle non-finite values.
Results may differ from the reference program's by a relative error of at most 0.0053.
Values may be sent and summed in bfloat16 or wider, within the bound.
A program may use at most 64 MiB of HBM per device.

```python
import math
import jax
import jax.numpy as jnp
from jax import lax

NO = 256
NE = 4
K1 = 32
K2 = 16
PAIRS = 65536


def block_levels(own_key, dims, cuts, low, largest):
    def one(position, parts):
        draws = jax.random.uniform(jax.random.fold_in(jax.random.fold_in(own_key, 6), position), (parts,), jnp.float32, low / len(cuts), largest / len(cuts))
        return jnp.repeat(jnp.exp(draws), dims[position] // parts).reshape((-1,) + (1,) * (len(dims) - position - 1))

    factor_of = one(*cuts[0])
    for cut in cuts[1:]:
        factor_of = factor_of * one(*cut)
    return factor_of


def noise(stream_key, shape, scale, reach, pieces=(), kind=jnp.bfloat16):
    level = block_levels(stream_key, shape, pieces, -0.22, 0.18) if pieces else 1.0
    array = jax.random.normal(stream_key, shape, jnp.float32) * scale * level
    return jnp.minimum(jnp.maximum(array, -reach), reach).astype(kind)


def setup_inputs(seed: int = 0) -> dict:
    key_of = jax.random.split(jax.random.key(seed), 3)
    return {
        "green": noise(key_of[0], (NE, 2, K1, K2, NO, NO), 1.0, 6.0, ((2, 32), (3, 8))),
        "screened": jnp.clip(0.1 + 0.9 * jax.random.uniform(key_of[1], (K1, K2, PAIRS), jnp.float32) ** block_levels(key_of[1], (K1, K2, PAIRS), ((2, 256),), -0.2, 0.2), 0.1, 1.0),
    }


full_turn = 2.0 * math.pi


def phase_tables(length, forward):
    step_counter = jnp.arange(length, dtype=jnp.int32)
    product = (step_counter[:, None] * step_counter[None, :]) % length
    angles = full_turn * product.astype(jnp.float32) / length
    if forward:
        return jnp.cos(angles) / length, jnp.sin(angles) / length
    return jnp.cos(angles), -jnp.sin(angles)


def apply_over_axis(matrix, values, along_dim):
    letters = "abcdefgh"[:values.ndim]
    target = letters[:along_dim] + "z" + letters[along_dim + 1:]
    formula = "z" + letters[along_dim] + "," + letters + "->" + target
    return jnp.einsum(formula, matrix, values, precision=lax.Precision.HIGHEST)


def complex_along(state, cosine, sine, along_dim):
    real_part, imag_part = state
    out_real = apply_over_axis(cosine, real_part, along_dim) - apply_over_axis(sine, imag_part, along_dim)
    out_imag = apply_over_axis(sine, real_part, along_dim) + apply_over_axis(cosine, imag_part, along_dim)
    return out_real, out_imag


def matmul_batch(left, right):
    return jnp.einsum('xyij,xyjl->xyil', left, right, precision=lax.Precision.HIGHEST)


def reference(green, screened):
    fwd_one = phase_tables(K1, True)
    fwd_two = phase_tables(K2, True)
    inv_one = phase_tables(K1, False)
    inv_two = phase_tables(K2, False)
    pair_weights = screened.reshape(K1, K2, NO, NO)
    green_rows = jnp.moveaxis(green, 4, 0)
    weight_rows = jnp.moveaxis(pair_weights, 2, 0)

    def one_row(operand_list):
        block, wblock = operand_list
        state = (block[:, 0].astype(jnp.float32), block[:, 1].astype(jnp.float32))
        state = complex_along(state, fwd_one[0], fwd_one[1], 1)
        state = complex_along(state, fwd_two[0], fwd_two[1], 2)
        state = (-wblock * state[0], -wblock * state[1])
        state = complex_along(state, inv_one[0], inv_one[1], 1)
        state = complex_along(state, inv_two[0], inv_two[1], 2)
        return jnp.stack(state, 1).astype(jnp.bfloat16)

    sigma = lax.map(one_row, (green_rows, weight_rows))
    sigma = jnp.moveaxis(sigma, 0, 4)

    def one_energy(operand_list):
        green_value_list, self_energy_values = operand_list
        green_real = green_value_list[0].astype(jnp.float32)
        green_imag = green_value_list[1].astype(jnp.float32)
        self_energy_real = self_energy_values[0].astype(jnp.float32)
        self_energy_imaginary = self_energy_values[1].astype(jnp.float32)
        kern_real = matmul_batch(green_real, self_energy_real) - matmul_batch(green_imag, self_energy_imaginary)
        kern_imag = matmul_batch(green_real, self_energy_imaginary) + matmul_batch(green_imag, self_energy_real)
        kern_real = lax.optimization_barrier(kern_real.astype(jnp.bfloat16)).astype(jnp.float32)
        kern_imag = lax.optimization_barrier(kern_imag.astype(jnp.bfloat16)).astype(jnp.float32)
        corr_real = matmul_batch(kern_real, green_real) - matmul_batch(kern_imag, green_imag)
        corr_imag = matmul_batch(kern_real, green_imag) + matmul_batch(kern_imag, green_real)
        return jnp.stack((green_real + corr_real / NO, green_imag + corr_imag / NO), 0).astype(jnp.bfloat16)

    dressed = lax.map(one_energy, (green, sigma))
    return sigma, dressed
```

```python
import math

import jax
import jax.numpy as jnp
from jax import lax
from jax.experimental import pallas as pl
from jax.experimental.pallas import tpu as pltpu
from jax.sharding import PartitionSpec as P

MESH = pl.DeviceIdType.MESH
HALVES = 2
SPLIT_TABLE = True
SINE = [(-1) ** n * (math.pi / 16) ** (2 * n + 1) / math.factorial(2 * n + 1) for n in range(7)]


def place():
    row, col = lax.axis_index("krow"), lax.axis_index("kcol")
    z, x_low, core = row // 4, (row // 2) % 2, row % 2
    x_high, y = col // 4, col % 4
    return row, col, z, x_high * 2 + x_low, y, core


def for_peers(visit):
    _, _, z, x, y, core = place()
    z_rows = [((z + dz) % 8) * 4 for dz in (4, 1, 7, 2, 6, 3, 5, 0)]

    def group(step, first):
        offset = (step * 13) % 32
        x_to, y_to, core_to = (x + offset // 8) % 4, (y + (offset // 2) % 4) % 4, (core + offset % 2) % 2
        low, col = (x_to % 2) * 2 + core_to, (x_to // 2) * 4 + y_to
        for z_row in z_rows[: 7 if first else 8]:
            visit(z_row + low, col)

    group(0, True)

    def body(step, carry):
        group(step, False)
        return carry

    lax.fori_loop(1, 32, body, 0)


def kernel(
    green_hbm, screened_hbm, sigma, dressed,
    green, weights, factors, wide, packed, landed, middle, back,
    table, table_low, states, weighted, load_sem, send_sem, recv_sem,
):
    row, col = place()[:2]
    me = row * 8 + col

    barrier = pltpu.get_barrier_semaphore()
    loads = [
        pltpu.make_async_copy(green_hbm.at[pl.ds(h * 8, 8)], green.at[pl.ds(h * 8, 8)], load_sem.at[h])
        for h in range(HALVES)
    ]
    loads += [
        pltpu.make_async_copy(
            screened_hbm.at[:, pl.ds(side * 128, 128)], weights.at[side], load_sem.at[2 + side]
        )
        for side in range(2)
    ]
    for load in loads:
        load.start()
    for_peers(lambda r, c: pl.semaphore_signal(barrier, inc=1, device_id=(r, c), device_id_type=MESH))

    def pack(h):
        for j in range(8):
            for side in range(2):
                part = green[h * 8 + j, :, pl.ds(side * 128, 128)]
                wide[side, pl.ds(j, 256, stride=8), :] = part.astype(jnp.float32)

        def body(i, carry):
            for side in range(2):
                rows = wide[side, pl.ds(i * 256, 256), :].reshape(32, 8, 128)
                packed[h, pl.ds(i * 32, 32), :, pl.ds(side * 128, 128)] = rows.astype(jnp.bfloat16)
            return carry

        lax.fori_loop(0, 8, body, 0)

    def send(source, target, h, lane):
        target[h, me] = source[h, me]

        def one(r, c):
            pltpu.make_async_remote_copy(
                source.at[h, r * 8 + c], target.at[h, me], send_sem.at[lane], recv_sem.at[lane],
                device_id=(r, c), device_id_type=MESH,
            ).start()

        for_peers(one)

    def arrive(source, target, h, lane):
        pltpu.make_async_remote_copy(
            source.at[h, pl.ds(0, 255)], target.at[h, pl.ds(0, 255)], send_sem.at[lane], recv_sem.at[lane],
            device_id=(row, col), device_id_type=MESH,
        ).wait_recv()

    def leave(source, target, h, lane):
        pltpu.make_async_remote_copy(
            source.at[h, pl.ds(0, 255)], target.at[h, pl.ds(0, 255)], send_sem.at[lane], recv_sem.at[lane],
            device_id=(row, col), device_id_type=MESH,
        ).wait_send()

    def fill_tables():
        r = lax.broadcasted_iota(jnp.int32, (32, 1024), 0)
        k = lax.broadcasted_iota(jnp.int32, (32, 1024), 1)
        r_two, r_part = (r // 4) * 2 + r % 2, (r // 2) % 2
        k_one, k_two, k_part = k // 32, ((k // 4) % 8) * 2 + k % 2, (k // 2) % 2
        start = 2 * k_two * r_two + 8 * (k_part - r_part) + 48

        def body(one, carry):
            turn = (start + one * k_one) % 32
            t = (8 - jnp.abs(turn - 16)).astype(jnp.float32)
            square = t * t
            value = jnp.full_like(t, SINE[6])
            for c in SINE[5::-1]:
                value = value * square + c
            value = value * t
            high = value.astype(jnp.bfloat16)
            at = pl.ds(one * 32, 32)
            table[at, :] = high
            if SPLIT_TABLE:
                table_low[at, :] = (value - high.astype(jnp.float32)).astype(jnp.bfloat16)
            return carry

        lax.fori_loop(0, 32, body, 0)

    def fill_factors():
        for side in range(2):
            for low in range(2):
                rows = weights[side, pl.ds(low, 256, stride=2), :] * (1.0 / 512)
                factors[side, pl.ds(low, 256, stride=4), :] = -rows
                factors[side, pl.ds(2 + low, 256, stride=4), :] = rows

    def times_table(at, operand):
        product = jnp.dot(table[at, :], operand[...], preferred_element_type=jnp.float32)
        if SPLIT_TABLE:
            product = product + jnp.dot(table_low[at, :], operand[...], preferred_element_type=jnp.float32)
        return product

    def convolve(h):
        upper = lax.broadcasted_iota(jnp.int32, (8, 8, 256), 1) < 4

        def gather(i, carry):
            rows = landed[h, pl.ds(i * 16, 16)].astype(jnp.float32).reshape(8, 2, 8, 256)
            even, odd = rows[:, 0], rows[:, 1]
            at = pl.ds(i * 64, 64)
            zero = jnp.where(upper, even, pltpu.roll(odd, 4, 1))
            one = jnp.where(upper, pltpu.roll(even, 4, 1), odd)
            states[at, pl.ds(0, 256)] = zero.reshape(64, 256).astype(jnp.bfloat16)
            states[at, pl.ds(256, 256)] = one.reshape(64, 256).astype(jnp.bfloat16)
            return carry

        lax.fori_loop(0, 16, gather, 0)

        def forward(i, carry):
            at = pl.ds(i * 256, 256)
            product = times_table(at, states)
            for q in range(4):
                part = product[:, q * 128 : (q + 1) * 128] * factors[q % 2, at, :]
                weighted[at, pl.ds(q * 128, 128)] = part.astype(jnp.bfloat16)
            return carry

        lax.fori_loop(0, 4, forward, 0)

        index = lax.broadcasted_iota(jnp.int32, (32, 8, 256), 1)
        sign = jnp.where((index // 2) % 2 == 0, 1.0, -1.0)

        def inverse(i, carry):
            product = times_table(pl.ds(i * 256, 256), weighted)
            zero = product[:, :256].reshape(32, 8, 256) * sign
            one = product[:, 256:].reshape(32, 8, 256) * sign
            even = jnp.where(index < 4, zero, pltpu.roll(one, 4, 1))
            odd = jnp.where(index < 4, pltpu.roll(zero, 4, 1), one)
            both = jnp.stack((even, odd), 1).reshape(64, 8, 256)
            middle[h, pl.ds(i * 64, 64)] = both.astype(jnp.bfloat16)
            return carry

        lax.fori_loop(0, 4, inverse, 0)

    def finish(h):
        def unpack(i, carry):
            for side in range(2):
                rows = back[h, pl.ds(i * 32, 32), :, pl.ds(side * 128, 128)].astype(jnp.float32)
                wide[side, pl.ds(i * 256, 256), :] = rows.reshape(256, 128)
            return carry

        lax.fori_loop(0, 8, unpack, 0)
        for j in range(8):
            for side in range(2):
                rows = wide[side, pl.ds(j, 256, stride=8), :]
                sigma[h * 8 + j, :, pl.ds(side * 128, 128)] = rows.astype(jnp.bfloat16)

        def dot(a, b):
            return jnp.dot(a, b, preferred_element_type=jnp.float32)

        def one(i, carry):
            real = h * 8 + (i // 2) * 4 + i % 2
            imag = real + 2
            g_real, g_imag, s_real, s_imag = green[real], green[imag], sigma[real], sigma[imag]
            k_real = (dot(g_real, s_real) - dot(g_imag, s_imag)).astype(jnp.bfloat16)
            k_imag = (dot(g_real, s_imag) + dot(g_imag, s_real)).astype(jnp.bfloat16)
            c_real = dot(k_real, g_real) - dot(k_imag, g_imag)
            c_imag = dot(k_real, g_imag) + dot(k_imag, g_real)
            dressed[real] = (g_real.astype(jnp.float32) + c_real * (1.0 / 256)).astype(jnp.bfloat16)
            dressed[imag] = (g_imag.astype(jnp.float32) + c_imag * (1.0 / 256)).astype(jnp.bfloat16)
            return carry

        lax.fori_loop(0, 4, one, 0)

    loads[0].wait()
    pack(0)
    pl.semaphore_wait(barrier, 255)
    send(packed, landed, 0, 0)
    loads[1].wait()
    pack(1)
    send(packed, landed, 1, 1)
    loads[2].wait()
    loads[3].wait()
    fill_factors()
    fill_tables()
    for h in range(HALVES):
        arrive(packed, landed, h, h)
        convolve(h)
        send(middle, back, h, 2 + h)
    for h in range(HALVES):
        arrive(middle, back, h, 2 + h)
        finish(h)
    for h in range(HALVES):
        leave(packed, landed, h, h)
        leave(middle, back, h, 2 + h)


def per_device(green, screened):
    blocks = pltpu.VMEM((HALVES, 256, 8, 256), jnp.bfloat16)
    matrices = jax.ShapeDtypeStruct((16, 256, 256), jnp.bfloat16)
    sigma, dressed = pl.pallas_call(
        kernel,
        out_shape=(matrices, matrices),
        in_specs=[pl.BlockSpec(memory_space=pl.ANY)] * 2,
        out_specs=[pl.BlockSpec(memory_space=pltpu.VMEM)] * 2,
        scratch_shapes=[
            pltpu.VMEM((16, 256, 256), jnp.bfloat16),
            pltpu.VMEM((2, 512, 128), jnp.float32),
            pltpu.VMEM((2, 1024, 128), jnp.float32),
            pltpu.VMEM((2, 2048, 128), jnp.float32),
            blocks,
            blocks,
            blocks,
            blocks,
            pltpu.VMEM((1024, 1024), jnp.bfloat16),
            pltpu.VMEM((1024, 1024), jnp.bfloat16),
            pltpu.VMEM((1024, 512), jnp.bfloat16),
            pltpu.VMEM((1024, 512), jnp.bfloat16),
            pltpu.SemaphoreType.DMA((4,)),
            pltpu.SemaphoreType.DMA((4,)),
            pltpu.SemaphoreType.DMA((4,)),
        ],
        compiler_params=pltpu.CompilerParams(
            collective_id=0, has_side_effects=True, vmem_limit_bytes=44 * 2**20
        ),
    )(green.reshape(16, 256, 256), screened.reshape(512, 256))
    return sigma.reshape(green.shape), dressed.reshape(green.shape)


def solution(mesh):
    spread = P(None, None, "krow", "kcol", None, None)
    return jax.shard_map(
        per_device,
        mesh=mesh,
        in_specs=(spread, P(None, None, ("krow", "kcol"))),
        out_specs=(spread, spread),
        check_vma=False,
    )
```

```python
import math

import jax
import jax.numpy as jnp
from jax import lax
from jax.experimental import pallas as pl
from jax.experimental.pallas import tpu as pltpu
from jax.sharding import PartitionSpec as P

MESH = pl.DeviceIdType.MESH
HALVES = 2
VMEM_LIMIT = 48 * 2**20
SPLIT_TABLE = True
SINE = [(-1) ** n * (math.pi / 16) ** (2 * n + 1) / math.factorial(2 * n + 1) for n in range(7)]


def place():
    row, col = lax.axis_index("krow"), lax.axis_index("kcol")
    z, x_low, core = row // 4, (row // 2) % 2, row % 2
    x_high, y = col // 4, col % 4
    return row, col, z, x_high * 2 + x_low, y, core


def for_peers(visit):
    _, _, z, x, y, core = place()
    z_rows = [((z + dz) % 8) * 4 for dz in (4, 1, 7, 2, 6, 3, 5, 0)]

    def group(step, first):
        offset = (step * 13) % 32
        x_to, y_to, core_to = (x + offset // 8) % 4, (y + (offset // 2) % 4) % 4, (core + offset % 2) % 2
        low, col = (x_to % 2) * 2 + core_to, (x_to // 2) * 4 + y_to
        for z_row in z_rows[: 7 if first else 8]:
            visit(z_row + low, col)

    group(0, True)

    def body(step, carry):
        group(step, False)
        return carry

    lax.fori_loop(1, 32, body, 0)


def for_peers_far_first(visit):
    _, _, z, x, y, core = place()
    z_rows = [((z + dz) % 8) * 4 for dz in range(8)]
    x_rows = [(((x + dx) % 4) % 2) * 2 for dx in range(4)]
    x_cols = [(((x + dx) % 4) // 2) * 4 for dx in range(4)]
    y_cols = [(y + dy) % 4 for dy in range(4)]
    cores = [core, 1 - core]
    steps = [0, 1, 2, 1]
    offsets = [(dz, dx, dy, dc) for dz in range(8) for dx in range(4) for dy in range(4) for dc in (1, 0)]
    offsets.sort(key=lambda o: (-min(o[0], 8 - o[0]) - steps[o[1]] - steps[o[2]], o))
    for dz, dx, dy, dc in offsets:
        if (dz, dx, dy, dc) != (0, 0, 0, 0):
            visit(z_rows[dz] + x_rows[dx] + cores[dc], x_cols[dx] + y_cols[dy])


def dot(a, b):
    return jnp.dot(a, b, preferred_element_type=jnp.float32)


def unpack(back, wide, sigma):
    def body(i, carry):
        for side in range(2):
            rows = back[pl.ds(i * 32, 32), :, pl.ds(side * 128, 128)].astype(jnp.float32)
            wide[side, pl.ds(i * 256, 256), :] = rows.reshape(256, 128)
        return carry

    lax.fori_loop(0, 8, body, 0)
    for j in range(8):
        for side in range(2):
            rows = wide[side, pl.ds(j, 256, stride=8), :]
            sigma[j, :, pl.ds(side * 128, 128)] = rows.astype(jnp.bfloat16)


def dress(green, sigma, dressed, real):
    imag = real + 2
    g_real, g_imag, s_real, s_imag = green[real], green[imag], sigma[real], sigma[imag]
    g_lower, g_swapped = jnp.concatenate((g_real, g_imag), 0), jnp.concatenate((g_imag, g_real), 0)
    k_real = dot(jnp.concatenate((g_real, -g_imag), 1), jnp.concatenate((s_real, s_imag), 0))
    k_imag = dot(jnp.concatenate((g_real, g_imag), 1), jnp.concatenate((s_imag, s_real), 0))
    k_real, k_imag = k_real.astype(jnp.bfloat16), k_imag.astype(jnp.bfloat16)
    c_real = dot(jnp.concatenate((k_real, -k_imag), 1), g_lower)
    c_imag = dot(jnp.concatenate((k_real, k_imag), 1), g_swapped)
    dressed[real] = (g_real.astype(jnp.float32) + c_real * (1.0 / 256)).astype(jnp.bfloat16)
    dressed[imag] = (g_imag.astype(jnp.float32) + c_imag * (1.0 / 256)).astype(jnp.bfloat16)


def kernel(
    green_hbm, screened_hbm, sigma, dressed, green, last,
    weights, factors, wide, packed, landed, middle, back,
    table, table_low, states, weighted, load_sem, send_sem, recv_sem,
):
    row, col = place()[:2]
    me = row * 8 + col

    barrier = pltpu.get_barrier_semaphore()
    loads = [
        pltpu.make_async_copy(green_hbm.at[pl.ds(h * 8, 8)], green.at[pl.ds(h * 8, 8)], load_sem.at[h])
        for h in range(HALVES)
    ]
    loads += [
        pltpu.make_async_copy(
            screened_hbm.at[:, pl.ds(side * 128, 128)], weights.at[side], load_sem.at[2 + side]
        )
        for side in range(2)
    ]
    for load in loads:
        load.start()
    with jax.named_scope("announce"):
        for_peers_far_first(lambda r, c: pl.semaphore_signal(barrier, inc=1, device_id=(r, c), device_id_type=MESH))

    def pack(h):
        for j in range(8):
            for side in range(2):
                part = green[h * 8 + j, :, pl.ds(side * 128, 128)]
                wide[side, pl.ds(j, 256, stride=8), :] = part.astype(jnp.float32)

        def body(i, carry):
            for side in range(2):
                rows = wide[side, pl.ds(i * 256, 256), :].reshape(32, 8, 128)
                packed[h, pl.ds(i * 32, 32), :, pl.ds(side * 128, 128)] = rows.astype(jnp.bfloat16)
            return carry

        lax.fori_loop(0, 8, body, 0)

    def send(source, target, lane):
        target[me] = source[me]

        def one(r, c):
            pltpu.make_async_remote_copy(
                source.at[r * 8 + c], target.at[me], send_sem.at[lane], recv_sem.at[lane],
                device_id=(r, c), device_id_type=MESH,
            ).start()

        for_peers(one)

    def whole(source, target, lane):
        return pltpu.make_async_remote_copy(
            source.at[pl.ds(0, 255)], target.at[pl.ds(0, 255)], send_sem.at[lane], recv_sem.at[lane],
            device_id=(row, col), device_id_type=MESH,
        )

    def fill_tables():
        r = lax.broadcasted_iota(jnp.int32, (32, 1024), 0)
        k = lax.broadcasted_iota(jnp.int32, (32, 1024), 1)
        r_two, r_part = (r // 4) * 2 + r % 2, (r // 2) % 2
        k_one, k_two, k_part = k // 32, ((k // 4) % 8) * 2 + k % 2, (k // 2) % 2
        start = 2 * k_two * r_two + 8 * (k_part - r_part) + 48

        def body(one, carry):
            turn = (start + one * k_one) % 32
            t = (8 - jnp.abs(turn - 16)).astype(jnp.float32)
            square = t * t
            value = jnp.full_like(t, SINE[6])
            for c in SINE[5::-1]:
                value = value * square + c
            value = value * t
            high = value.astype(jnp.bfloat16)
            at = pl.ds(one * 32, 32)
            table[at, :] = high
            if SPLIT_TABLE:
                table_low[at, :] = (value - high.astype(jnp.float32)).astype(jnp.bfloat16)
            return carry

        lax.fori_loop(0, 32, body, 0)

    def fill_factors():
        for side in range(2):
            for low in range(2):
                rows = weights[side, pl.ds(low, 256, stride=2), :] * (1.0 / 512)
                factors[side, pl.ds(low, 256, stride=4), :] = -rows
                factors[side, pl.ds(2 + low, 256, stride=4), :] = rows

    def times_table(at, operand):
        product = jnp.dot(table[at, :], operand[...], preferred_element_type=jnp.float32)
        if SPLIT_TABLE:
            product = product + jnp.dot(table_low[at, :], operand[...], preferred_element_type=jnp.float32)
        return product

    def convolve(h):
        upper = lax.broadcasted_iota(jnp.int32, (8, 8, 256), 1) < 4

        def gather(i, carry):
            rows = landed[h, pl.ds(i * 16, 16)].astype(jnp.float32).reshape(8, 2, 8, 256)
            even, odd = rows[:, 0], rows[:, 1]
            at = pl.ds(i * 64, 64)
            zero = jnp.where(upper, even, pltpu.roll(odd, 4, 1))
            one = jnp.where(upper, pltpu.roll(even, 4, 1), odd)
            states[at, pl.ds(0, 256)] = zero.reshape(64, 256).astype(jnp.bfloat16)
            states[at, pl.ds(256, 256)] = one.reshape(64, 256).astype(jnp.bfloat16)
            return carry

        lax.fori_loop(0, 16, gather, 0)

        def forward(i, carry):
            at = pl.ds(i * 256, 256)
            product = times_table(at, states)
            for q in range(4):
                part = product[:, q * 128 : (q + 1) * 128] * factors[q % 2, at, :]
                weighted[at, pl.ds(q * 128, 128)] = part.astype(jnp.bfloat16)
            return carry

        lax.fori_loop(0, 4, forward, 0)

        index = lax.broadcasted_iota(jnp.int32, (32, 8, 256), 1)
        sign = jnp.where((index // 2) % 2 == 0, 1.0, -1.0)

        def inverse(i, carry):
            product = times_table(pl.ds(i * 256, 256), weighted)
            zero = product[:, :256].reshape(32, 8, 256) * sign
            one = product[:, 256:].reshape(32, 8, 256) * sign
            even = jnp.where(index < 4, zero, pltpu.roll(one, 4, 1))
            odd = jnp.where(index < 4, pltpu.roll(zero, 4, 1), one)
            both = jnp.stack((even, odd), 1).reshape(64, 8, 256)
            middle[h, pl.ds(i * 64, 64)] = both.astype(jnp.bfloat16)
            return carry

        lax.fori_loop(0, 4, inverse, 0)

    def finish():
        unpack(back, wide, sigma)

        def one(i, carry):
            dress(green, sigma, dressed, (i // 2) * 4 + i % 2)
            return carry

        lax.fori_loop(0, 4, one, 0)

    scope = jax.named_scope
    with scope("load0"):
        loads[0].wait()
    with scope("pack0"):
        pack(0)
    with scope("barrier"):
        pl.semaphore_wait(barrier, 255)
    moves = [(packed.at[h], landed.at[h], h) for h in range(HALVES)]
    moves += [(middle.at[h], (back, last)[h], 2 + h) for h in range(HALVES)]
    with scope("send0"):
        send(*moves[0])
    with scope("load1"):
        loads[1].wait()
    with scope("pack1"):
        pack(1)
    with scope("send1"):
        send(*moves[1])
    with scope("factors"):
        loads[2].wait()
        loads[3].wait()
        fill_factors()
    with scope("tables"):
        fill_tables()
    for h in range(HALVES):
        with scope(f"arrive{h}"):
            whole(*moves[h]).wait_recv()
        with scope(f"convolve{h}"):
            convolve(h)
        with scope(f"return{h}"):
            send(*moves[2 + h])
    with scope("back0"):
        whole(*moves[2]).wait_recv()
    with scope("finish0"):
        finish()
    with scope("back1"):
        whole(*moves[3]).wait_recv()
    with scope("leave"):
        for move in moves:
            whole(*move).wait_send()


def closing(
    sigma_half, dressed_half, green, last, sigma_hbm, dressed_hbm, wide, sigma, dressed, copy_sem
):
    def copy(source, target, part, lane):
        return pltpu.make_async_copy(source, target.at[pl.ds(part, source.shape[0])], copy_sem.at[lane])

    copies = [copy(sigma_half, sigma_hbm, 0, 0), copy(dressed_half, dressed_hbm, 0, 1)]
    for c in copies:
        c.start()
    with jax.named_scope("unpack"):
        unpack(last, wide, sigma)
    copies.append(copy(sigma, sigma_hbm, 8, 2))
    copies[-1].start()
    for n in range(4):
        real = (n // 2) * 4 + n % 2
        with jax.named_scope(f"dress{n}"):
            dress(green.at[pl.ds(8, 8)], sigma, dressed, real)
        for part in (real, real + 2):
            copies.append(copy(dressed.at[pl.ds(part, 1)], dressed_hbm, 8 + part, 3 + part))
            copies[-1].start()
    with jax.named_scope("drain"):
        for c in copies:
            c.wait()


def per_device(green, screened):
    vmem = pl.BlockSpec(memory_space=pltpu.VMEM)
    hbm = pl.BlockSpec(memory_space=pltpu.HBM)
    blocks = pltpu.VMEM((HALVES, 256, 8, 256), jnp.bfloat16)
    half = jax.ShapeDtypeStruct((8, 256, 256), jnp.bfloat16)
    matrices = jax.ShapeDtypeStruct((16, 256, 256), jnp.bfloat16)
    wide = pltpu.VMEM((2, 2048, 128), jnp.float32)
    parts = pl.pallas_call(
        kernel,
        out_shape=(half, half, matrices, jax.ShapeDtypeStruct((256, 8, 256), jnp.bfloat16)),
        in_specs=[hbm] * 2,
        out_specs=[vmem] * 4,
        scratch_shapes=[
            pltpu.VMEM((2, 512, 128), jnp.float32),
            pltpu.VMEM((2, 1024, 128), jnp.float32),
            wide,
            blocks,
            blocks,
            blocks,
            pltpu.VMEM((256, 8, 256), jnp.bfloat16),
            pltpu.VMEM((1024, 1024), jnp.bfloat16),
            pltpu.VMEM((1024, 1024), jnp.bfloat16),
            pltpu.VMEM((1024, 512), jnp.bfloat16),
            pltpu.VMEM((1024, 512), jnp.bfloat16),
            pltpu.SemaphoreType.DMA((4,)),
            pltpu.SemaphoreType.DMA((4,)),
            pltpu.SemaphoreType.DMA((4,)),
        ],
        compiler_params=pltpu.CompilerParams(
            collective_id=0, has_side_effects=True, vmem_limit_bytes=VMEM_LIMIT
        ),
    )(green.reshape(16, 256, 256), pltpu.with_memory_space_constraint(screened.reshape(512, 256), pltpu.HBM))
    sigma, dressed = pl.pallas_call(
        closing,
        out_shape=(matrices, matrices),
        in_specs=[vmem] * 4,
        out_specs=[hbm] * 2,
        scratch_shapes=[
            wide,
            pltpu.VMEM((8, 256, 256), jnp.bfloat16),
            pltpu.VMEM((8, 256, 256), jnp.bfloat16),
            pltpu.SemaphoreType.DMA((11,)),
        ],
        compiler_params=pltpu.CompilerParams(vmem_limit_bytes=16 * 2**20),
    )(*parts)
    return sigma.reshape(green.shape), dressed.reshape(green.shape)


def solution(mesh):
    spread = P(None, None, "krow", "kcol", None, None)
    return jax.shard_map(
        per_device,
        mesh=mesh,
        in_specs=(spread, P(None, None, ("krow", "kcol"))),
        out_specs=(spread, spread),
        check_vma=False,
    )
```

```python
import math

import jax
import jax.numpy as jnp
from jax import lax
from jax.experimental import pallas as pl
from jax.experimental.pallas import tpu as pltpu
from jax.sharding import PartitionSpec as P

MESH = pl.DeviceIdType.MESH
HALVES = 2
VMEM_LIMIT = 48 * 2**20
SPLIT_TABLE = True
SINE = [(-1) ** n * (math.pi / 16) ** (2 * n + 1) / math.factorial(2 * n + 1) for n in range(7)]


def place():
    row, col = lax.axis_index("krow"), lax.axis_index("kcol")
    z, x_low, core = row // 4, (row // 2) % 2, row % 2
    x_high, y = col // 4, col % 4
    return row, col, z, x_high * 2 + x_low, y, core


def for_peers(visit):
    _, _, z, x, y, core = place()
    z_rows = [((z + dz) % 8) * 4 for dz in (4, 1, 7, 2, 6, 3, 5, 0)]

    def group(step, first):
        x_to, y_to, core_to = (x + step // 8) % 4, (y + (step // 2) % 4) % 4, (core + step % 2) % 2
        low, col = (x_to % 2) * 2 + core_to, (x_to // 2) * 4 + y_to
        for z_row in z_rows[: 7 if first else 8]:
            visit(z_row + low, col)

    group(0, True)

    def body(step, carry):
        group(step, False)
        return carry

    lax.fori_loop(1, 32, body, 0)


def for_peers_far_first(visit):
    _, _, z, x, y, core = place()
    z_rows = [((z + dz) % 8) * 4 for dz in range(8)]
    x_rows = [(((x + dx) % 4) % 2) * 2 for dx in range(4)]
    x_cols = [(((x + dx) % 4) // 2) * 4 for dx in range(4)]
    y_cols = [(y + dy) % 4 for dy in range(4)]
    cores = [core, 1 - core]
    steps = [0, 1, 2, 1]
    offsets = [(dz, dx, dy, dc) for dz in range(8) for dx in range(4) for dy in range(4) for dc in (1, 0)]
    offsets.sort(key=lambda o: (-min(o[0], 8 - o[0]) - steps[o[1]] - steps[o[2]], o))
    for dz, dx, dy, dc in offsets:
        if (dz, dx, dy, dc) != (0, 0, 0, 0):
            visit(z_rows[dz] + x_rows[dx] + cores[dc], x_cols[dx] + y_cols[dy])


def dot(a, b):
    return jnp.dot(a, b, preferred_element_type=jnp.float32)


def unpack(back, wide, sigma):
    def body(i, carry):
        for side in range(2):
            rows = back[pl.ds(i * 32, 32), :, pl.ds(side * 128, 128)].astype(jnp.float32)
            wide[side, pl.ds(i * 256, 256), :] = rows.reshape(256, 128)
        return carry

    lax.fori_loop(0, 8, body, 0)
    for j in range(8):
        for side in range(2):
            rows = wide[side, pl.ds(j, 256, stride=8), :]
            sigma[j, :, pl.ds(side * 128, 128)] = rows.astype(jnp.bfloat16)


def dress(green, sigma, dressed, real):
    imag = real + 2
    g_real, g_imag, s_real, s_imag = green[real], green[imag], sigma[real], sigma[imag]
    g_lower, g_swapped = jnp.concatenate((g_real, g_imag), 0), jnp.concatenate((g_imag, g_real), 0)
    k_real = dot(jnp.concatenate((g_real, -g_imag), 1), jnp.concatenate((s_real, s_imag), 0))
    k_imag = dot(jnp.concatenate((g_real, g_imag), 1), jnp.concatenate((s_imag, s_real), 0))
    k_real, k_imag = k_real.astype(jnp.bfloat16), k_imag.astype(jnp.bfloat16)
    c_real = dot(jnp.concatenate((k_real, -k_imag), 1), g_lower)
    c_imag = dot(jnp.concatenate((k_real, k_imag), 1), g_swapped)
    dressed[real] = (g_real.astype(jnp.float32) + c_real * (1.0 / 256)).astype(jnp.bfloat16)
    dressed[imag] = (g_imag.astype(jnp.float32) + c_imag * (1.0 / 256)).astype(jnp.bfloat16)


def kernel(
    green_hbm, screened_hbm, sigma, dressed, green, last,
    weights, factors, wide, packed, landed, middle, back,
    table, table_low, states, weighted, load_sem, send_sem, recv_sem,
):
    row, col = place()[:2]
    me = row * 8 + col

    barrier = pltpu.get_barrier_semaphore()
    loads = [
        pltpu.make_async_copy(green_hbm.at[pl.ds(h * 8, 8)], green.at[pl.ds(h * 8, 8)], load_sem.at[h])
        for h in range(HALVES)
    ]
    loads += [
        pltpu.make_async_copy(
            screened_hbm.at[:, pl.ds(side * 128, 128)], weights.at[side], load_sem.at[2 + side]
        )
        for side in range(2)
    ]
    for load in loads:
        load.start()
    with jax.named_scope("announce"):
        for_peers_far_first(lambda r, c: pl.semaphore_signal(barrier, inc=1, device_id=(r, c), device_id_type=MESH))

    def pack(h):
        for j in range(8):
            for side in range(2):
                part = green[h * 8 + j, :, pl.ds(side * 128, 128)]
                wide[side, pl.ds(j, 256, stride=8), :] = part.astype(jnp.float32)

        def body(i, carry):
            for side in range(2):
                rows = wide[side, pl.ds(i * 256, 256), :].reshape(32, 8, 128)
                packed[h, pl.ds(i * 32, 32), :, pl.ds(side * 128, 128)] = rows.astype(jnp.bfloat16)
            return carry

        lax.fori_loop(0, 8, body, 0)

    def send(source, target, lane):
        target[me] = source[me]

        def one(r, c):
            pltpu.make_async_remote_copy(
                source.at[r * 8 + c], target.at[me], send_sem.at[lane], recv_sem.at[lane],
                device_id=(r, c), device_id_type=MESH,
            ).start()

        for_peers(one)

    def whole(source, target, lane):
        return pltpu.make_async_remote_copy(
            source.at[pl.ds(0, 255)], target.at[pl.ds(0, 255)], send_sem.at[lane], recv_sem.at[lane],
            device_id=(row, col), device_id_type=MESH,
        )

    def fill_tables():
        r = lax.broadcasted_iota(jnp.int32, (32, 1024), 0)
        k = lax.broadcasted_iota(jnp.int32, (32, 1024), 1)
        r_two, r_part = (r // 4) * 2 + r % 2, (r // 2) % 2
        k_one, k_two, k_part = k // 32, ((k // 4) % 8) * 2 + k % 2, (k // 2) % 2
        start = 2 * k_two * r_two + 8 * (k_part - r_part) + 48

        def body(one, carry):
            turn = (start + one * k_one) % 32
            t = (8 - jnp.abs(turn - 16)).astype(jnp.float32)
            square = t * t
            value = jnp.full_like(t, SINE[6])
            for c in SINE[5::-1]:
                value = value * square + c
            value = value * t
            high = value.astype(jnp.bfloat16)
            at = pl.ds(one * 32, 32)
            table[at, :] = high
            if SPLIT_TABLE:
                table_low[at, :] = (value - high.astype(jnp.float32)).astype(jnp.bfloat16)
            return carry

        lax.fori_loop(0, 32, body, 0)

    def fill_factors():
        for side in range(2):
            for low in range(2):
                rows = weights[side, pl.ds(low, 256, stride=2), :] * (1.0 / 512)
                factors[side, pl.ds(low, 256, stride=4), :] = -rows
                factors[side, pl.ds(2 + low, 256, stride=4), :] = rows

    def times_table(at, operand):
        product = jnp.dot(table[at, :], operand[...], preferred_element_type=jnp.float32)
        if SPLIT_TABLE:
            product = product + jnp.dot(table_low[at, :], operand[...], preferred_element_type=jnp.float32)
        return product

    def convolve(h):
        upper = lax.broadcasted_iota(jnp.int32, (8, 8, 256), 1) < 4

        def gather(i, carry):
            rows = landed[h, pl.ds(i * 16, 16)].astype(jnp.float32).reshape(8, 2, 8, 256)
            even, odd = rows[:, 0], rows[:, 1]
            at = pl.ds(i * 64, 64)
            zero = jnp.where(upper, even, pltpu.roll(odd, 4, 1))
            one = jnp.where(upper, pltpu.roll(even, 4, 1), odd)
            states[at, pl.ds(0, 256)] = zero.reshape(64, 256).astype(jnp.bfloat16)
            states[at, pl.ds(256, 256)] = one.reshape(64, 256).astype(jnp.bfloat16)
            return carry

        lax.fori_loop(0, 16, gather, 0)

        def forward(i, carry):
            at = pl.ds(i * 256, 256)
            product = times_table(at, states)
            for q in range(4):
                part = product[:, q * 128 : (q + 1) * 128] * factors[q % 2, at, :]
                weighted[at, pl.ds(q * 128, 128)] = part.astype(jnp.bfloat16)
            return carry

        lax.fori_loop(0, 4, forward, 0)

        index = lax.broadcasted_iota(jnp.int32, (32, 8, 256), 1)
        sign = jnp.where((index // 2) % 2 == 0, 1.0, -1.0)

        def inverse(i, carry):
            product = times_table(pl.ds(i * 256, 256), weighted)
            zero = product[:, :256].reshape(32, 8, 256) * sign
            one = product[:, 256:].reshape(32, 8, 256) * sign
            even = jnp.where(index < 4, zero, pltpu.roll(one, 4, 1))
            odd = jnp.where(index < 4, pltpu.roll(zero, 4, 1), one)
            both = jnp.stack((even, odd), 1).reshape(64, 8, 256)
            middle[h, pl.ds(i * 64, 64)] = both.astype(jnp.bfloat16)
            return carry

        lax.fori_loop(0, 4, inverse, 0)

    def finish():
        unpack(back, wide, sigma)

        def one(i, carry):
            dress(green, sigma, dressed, (i // 2) * 4 + i % 2)
            return carry

        lax.fori_loop(0, 4, one, 0)

    scope = jax.named_scope
    with scope("load0"):
        loads[0].wait()
    with scope("pack0"):
        pack(0)
    with scope("barrier"):
        pl.semaphore_wait(barrier, 255)
    moves = [(packed.at[h], landed.at[h], h) for h in range(HALVES)]
    moves += [(middle.at[h], (back, last)[h], 2 + h) for h in range(HALVES)]
    with scope("send0"):
        send(*moves[0])
    with scope("load1"):
        loads[1].wait()
    with scope("pack1"):
        pack(1)
    with scope("send1"):
        send(*moves[1])
    with scope("factors"):
        loads[2].wait()
        loads[3].wait()
        fill_factors()
    with scope("tables"):
        fill_tables()
    for h in range(HALVES):
        with scope(f"arrive{h}"):
            whole(*moves[h]).wait_recv()
        with scope(f"convolve{h}"):
            convolve(h)
        with scope(f"return{h}"):
            send(*moves[2 + h])
    with scope("back0"):
        whole(*moves[2]).wait_recv()
    with scope("finish0"):
        finish()
    with scope("back1"):
        whole(*moves[3]).wait_recv()
    with scope("leave"):
        for move in moves:
            whole(*move).wait_send()


def closing(
    sigma_half, dressed_half, green, last, sigma_hbm, dressed_hbm, wide, sigma, dressed, copy_sem
):
    def copy(source, target, part, lane):
        return pltpu.make_async_copy(source, target.at[pl.ds(part, source.shape[0])], copy_sem.at[lane])

    copies = [copy(sigma_half, sigma_hbm, 0, 0), copy(dressed_half, dressed_hbm, 0, 1)]
    for c in copies:
        c.start()
    with jax.named_scope("unpack"):
        unpack(last, wide, sigma)
    copies.append(copy(sigma, sigma_hbm, 8, 2))
    copies[-1].start()
    for n in range(4):
        real = (n // 2) * 4 + n % 2
        with jax.named_scope(f"dress{n}"):
            dress(green.at[pl.ds(8, 8)], sigma, dressed, real)
        for part in (real, real + 2):
            copies.append(copy(dressed.at[pl.ds(part, 1)], dressed_hbm, 8 + part, 3 + part))
            copies[-1].start()
    with jax.named_scope("drain"):
        for c in copies:
            c.wait()


def per_device(green, screened):
    vmem = pl.BlockSpec(memory_space=pltpu.VMEM)
    hbm = pl.BlockSpec(memory_space=pltpu.HBM)
    blocks = pltpu.VMEM((HALVES, 256, 8, 256), jnp.bfloat16)
    half = jax.ShapeDtypeStruct((8, 256, 256), jnp.bfloat16)
    matrices = jax.ShapeDtypeStruct((16, 256, 256), jnp.bfloat16)
    wide = pltpu.VMEM((2, 2048, 128), jnp.float32)
    parts = pl.pallas_call(
        kernel,
        out_shape=(half, half, matrices, jax.ShapeDtypeStruct((256, 8, 256), jnp.bfloat16)),
        in_specs=[hbm] * 2,
        out_specs=[vmem] * 4,
        scratch_shapes=[
            pltpu.VMEM((2, 512, 128), jnp.float32),
            pltpu.VMEM((2, 1024, 128), jnp.float32),
            wide,
            blocks,
            blocks,
            blocks,
            pltpu.VMEM((256, 8, 256), jnp.bfloat16),
            pltpu.VMEM((1024, 1024), jnp.bfloat16),
            pltpu.VMEM((1024, 1024), jnp.bfloat16),
            pltpu.VMEM((1024, 512), jnp.bfloat16),
            pltpu.VMEM((1024, 512), jnp.bfloat16),
            pltpu.SemaphoreType.DMA((4,)),
            pltpu.SemaphoreType.DMA((4,)),
            pltpu.SemaphoreType.DMA((4,)),
        ],
        compiler_params=pltpu.CompilerParams(
            collective_id=0, has_side_effects=True, vmem_limit_bytes=VMEM_LIMIT
        ),
    )(green.reshape(16, 256, 256), pltpu.with_memory_space_constraint(screened.reshape(512, 256), pltpu.HBM))
    sigma, dressed = pl.pallas_call(
        closing,
        out_shape=(matrices, matrices),
        in_specs=[vmem] * 4,
        out_specs=[hbm] * 2,
        scratch_shapes=[
            wide,
            pltpu.VMEM((8, 256, 256), jnp.bfloat16),
            pltpu.VMEM((8, 256, 256), jnp.bfloat16),
            pltpu.SemaphoreType.DMA((11,)),
        ],
        compiler_params=pltpu.CompilerParams(vmem_limit_bytes=16 * 2**20),
    )(*parts)
    return sigma.reshape(green.shape), dressed.reshape(green.shape)


def solution(mesh):
    spread = P(None, None, "krow", "kcol", None, None)
    return jax.shard_map(
        per_device,
        mesh=mesh,
        in_specs=(spread, P(None, None, ("krow", "kcol"))),
        out_specs=(spread, spread),
        check_vma=False,
    )
```

```python
import math

import jax
import jax.numpy as jnp
from jax import lax
from jax.experimental import pallas as pl
from jax.experimental.pallas import tpu as pltpu
from jax.sharding import PartitionSpec as P

MESH = pl.DeviceIdType.MESH
HALVES = 2
VMEM_LIMIT = 48 * 2**20
SPLIT_TABLE = True
SINE = [(-1) ** n * (math.pi / 16) ** (2 * n + 1) / math.factorial(2 * n + 1) for n in range(7)]


def place():
    row, col = lax.axis_index("krow"), lax.axis_index("kcol")
    z, x_low, core = row // 4, (row // 2) % 2, row % 2
    x_high, y = col // 4, col % 4
    return row, col, z, x_high * 2 + x_low, y, core


def for_peers(visit):
    _, _, z, x, y, core = place()
    z_rows = [((z + dz) % 8) * 4 for dz in (4, 1, 7, 2, 6, 3, 5, 0)]

    def group(step, first):
        x_to, y_to, core_to = (x + step // 8) % 4, (y + (step // 2) % 4) % 4, (core + step % 2) % 2
        low, col = (x_to % 2) * 2 + core_to, (x_to // 2) * 4 + y_to
        for z_row in z_rows[: 7 if first else 8]:
            visit(z_row + low, col)

    group(0, True)

    def body(step, carry):
        group(step, False)
        return carry

    lax.fori_loop(1, 32, body, 0)


def for_peers_far_first(visit):
    _, _, z, x, y, core = place()
    z_rows = [((z + dz) % 8) * 4 for dz in range(8)]
    x_rows = [(((x + dx) % 4) % 2) * 2 for dx in range(4)]
    x_cols = [(((x + dx) % 4) // 2) * 4 for dx in range(4)]
    y_cols = [(y + dy) % 4 for dy in range(4)]
    cores = [core, 1 - core]
    steps = [0, 1, 2, 1]
    offsets = [(dz, dx, dy, dc) for dz in range(8) for dx in range(4) for dy in range(4) for dc in (1, 0)]
    offsets.sort(key=lambda o: (-min(o[0], 8 - o[0]) - steps[o[1]] - steps[o[2]], o))
    for dz, dx, dy, dc in offsets:
        if (dz, dx, dy, dc) != (0, 0, 0, 0):
            visit(z_rows[dz] + x_rows[dx] + cores[dc], x_cols[dx] + y_cols[dy])


def dot(a, b):
    return jnp.dot(a, b, preferred_element_type=jnp.float32)


def unpack(back, wide, sigma):
    def body(i, carry):
        for side in range(2):
            rows = back[pl.ds(i * 32, 32), :, pl.ds(side * 128, 128)].astype(jnp.float32)
            wide[side, pl.ds(i * 256, 256), :] = rows.reshape(256, 128)
        return carry

    lax.fori_loop(0, 8, body, 0)
    for j in range(8):
        for side in range(2):
            rows = wide[side, pl.ds(j, 256, stride=8), :]
            sigma[j, :, pl.ds(side * 128, 128)] = rows.astype(jnp.bfloat16)


def dress(green, sigma, dressed, real):
    imag = real + 2
    g_real, g_imag, s_real, s_imag = green[real], green[imag], sigma[real], sigma[imag]
    g_lower, g_swapped = jnp.concatenate((g_real, g_imag), 0), jnp.concatenate((g_imag, g_real), 0)
    k_real = dot(jnp.concatenate((g_real, -g_imag), 1), jnp.concatenate((s_real, s_imag), 0))
    k_imag = dot(jnp.concatenate((g_real, g_imag), 1), jnp.concatenate((s_imag, s_real), 0))
    k_real, k_imag = k_real.astype(jnp.bfloat16), k_imag.astype(jnp.bfloat16)
    c_real = dot(jnp.concatenate((k_real, -k_imag), 1), g_lower)
    c_imag = dot(jnp.concatenate((k_real, k_imag), 1), g_swapped)
    dressed[real] = (g_real.astype(jnp.float32) + c_real * (1.0 / 256)).astype(jnp.bfloat16)
    dressed[imag] = (g_imag.astype(jnp.float32) + c_imag * (1.0 / 256)).astype(jnp.bfloat16)


def kernel(
    green_hbm, screened_hbm, sigma, dressed, green, last,
    weights, factors, wide, packed, landed, middle, back,
    table, table_low, states, weighted, load_sem, send_sem, recv_sem,
):
    row, col = place()[:2]
    me = row * 8 + col

    barrier = pltpu.get_barrier_semaphore()
    loads = [
        pltpu.make_async_copy(green_hbm.at[pl.ds(h * 8, 8)], green.at[pl.ds(h * 8, 8)], load_sem.at[h])
        for h in range(HALVES)
    ]
    loads += [
        pltpu.make_async_copy(
            screened_hbm.at[:, pl.ds(side * 128, 128)], weights.at[side], load_sem.at[2 + side]
        )
        for side in range(2)
    ]
    for load in loads:
        load.start()
    with jax.named_scope("announce"):
        for_peers_far_first(lambda r, c: pl.semaphore_signal(barrier, inc=1, device_id=(r, c), device_id_type=MESH))

    def pack(h):
        for j in range(8):
            for side in range(2):
                part = green[h * 8 + j, :, pl.ds(side * 128, 128)]
                wide[side, pl.ds(j, 256, stride=8), :] = part.astype(jnp.float32)

        def body(i, carry):
            for side in range(2):
                rows = wide[side, pl.ds(i * 256, 256), :].reshape(32, 8, 128)
                packed[h, pl.ds(i * 32, 32), :, pl.ds(side * 128, 128)] = rows.astype(jnp.bfloat16)
            return carry

        lax.fori_loop(0, 8, body, 0)

    def send(source, target, lane):
        target[me] = source[me]

        def one(r, c):
            pltpu.make_async_remote_copy(
                source.at[r * 8 + c], target.at[me], send_sem.at[lane], recv_sem.at[lane],
                device_id=(r, c), device_id_type=MESH,
            ).start()

        for_peers(one)

    def whole(source, target, lane):
        return pltpu.make_async_remote_copy(
            source.at[pl.ds(0, 255)], target.at[pl.ds(0, 255)], send_sem.at[lane], recv_sem.at[lane],
            device_id=(row, col), device_id_type=MESH,
        )

    def fill_tables():
        r = lax.broadcasted_iota(jnp.int32, (32, 1024), 0)
        k = lax.broadcasted_iota(jnp.int32, (32, 1024), 1)
        r_two, r_part = (r // 4) * 2 + r % 2, (r // 2) % 2
        k_one, k_two, k_part = k // 32, ((k // 4) % 8) * 2 + k % 2, (k // 2) % 2
        start = 2 * k_two * r_two + 8 * (k_part - r_part) + 48

        def body(one, carry):
            turn = (start + one * k_one) % 32
            t = (8 - jnp.abs(turn - 16)).astype(jnp.float32)
            square = t * t
            value = jnp.full_like(t, SINE[6])
            for c in SINE[5::-1]:
                value = value * square + c
            value = value * t
            high = value.astype(jnp.bfloat16)
            at = pl.ds(one * 32, 32)
            table[at, :] = high
            if SPLIT_TABLE:
                table_low[at, :] = (value - high.astype(jnp.float32)).astype(jnp.bfloat16)
            return carry

        lax.fori_loop(0, 32, body, 0)

    def fill_factors():
        for side in range(2):
            for low in range(2):
                rows = weights[side, pl.ds(low, 256, stride=2), :] * (1.0 / 512)
                factors[side, pl.ds(low, 256, stride=4), :] = -rows
                factors[side, pl.ds(2 + low, 256, stride=4), :] = rows

    def times_table(at, operand):
        product = jnp.dot(table[at, :], operand[...], preferred_element_type=jnp.float32)
        if SPLIT_TABLE:
            product = product + jnp.dot(table_low[at, :], operand[...], preferred_element_type=jnp.float32)
        return product

    def convolve(h):
        upper = lax.broadcasted_iota(jnp.int32, (8, 8, 256), 1) < 4

        def gather(i, carry):
            rows = landed[h, pl.ds(i * 16, 16)].astype(jnp.float32).reshape(8, 2, 8, 256)
            even, odd = rows[:, 0], rows[:, 1]
            at = pl.ds(i * 64, 64)
            zero = jnp.where(upper, even, pltpu.roll(odd, 4, 1))
            one = jnp.where(upper, pltpu.roll(even, 4, 1), odd)
            states[at, pl.ds(0, 256)] = zero.reshape(64, 256).astype(jnp.bfloat16)
            states[at, pl.ds(256, 256)] = one.reshape(64, 256).astype(jnp.bfloat16)
            return carry

        lax.fori_loop(0, 16, gather, 0)

        def forward(i, carry):
            at = pl.ds(i * 256, 256)
            product = times_table(at, states)
            for q in range(4):
                part = product[:, q * 128 : (q + 1) * 128] * factors[q % 2, at, :]
                weighted[at, pl.ds(q * 128, 128)] = part.astype(jnp.bfloat16)
            return carry

        lax.fori_loop(0, 4, forward, 0)

        index = lax.broadcasted_iota(jnp.int32, (32, 8, 256), 1)
        sign = jnp.where((index // 2) % 2 == 0, 1.0, -1.0)

        def inverse(i, carry):
            product = times_table(pl.ds(i * 256, 256), weighted)
            zero = product[:, :256].reshape(32, 8, 256) * sign
            one = product[:, 256:].reshape(32, 8, 256) * sign
            even = jnp.where(index < 4, zero, pltpu.roll(one, 4, 1))
            odd = jnp.where(index < 4, pltpu.roll(zero, 4, 1), one)
            both = jnp.stack((even, odd), 1).reshape(64, 8, 256)
            middle[h, pl.ds(i * 64, 64)] = both.astype(jnp.bfloat16)
            return carry

        lax.fori_loop(0, 4, inverse, 0)

    def finish():
        unpack(back, wide, sigma)

        def one(i, carry):
            dress(green, sigma, dressed, (i // 2) * 4 + i % 2)
            return carry

        lax.fori_loop(0, 4, one, 0)

    scope = jax.named_scope
    with scope("load0"):
        loads[0].wait()
    with scope("pack0"):
        pack(0)
    with scope("barrier"):
        pl.semaphore_wait(barrier, 255)
    moves = [(packed.at[h], landed.at[h], h) for h in range(HALVES)]
    moves += [(middle.at[h], (back, last)[h], 2 + h) for h in range(HALVES)]
    with scope("send0"):
        send(*moves[0])
    with scope("load1"):
        loads[1].wait()
    with scope("pack1"):
        pack(1)
    with scope("send1"):
        send(*moves[1])
    with scope("factors"):
        loads[2].wait()
        loads[3].wait()
        fill_factors()
    with scope("tables"):
        fill_tables()
    for h in range(HALVES):
        with scope(f"arrive{h}"):
            whole(*moves[h]).wait_recv()
        with scope(f"convolve{h}"):
            convolve(h)
        with scope(f"return{h}"):
            send(*moves[2 + h])
    with scope("back0"):
        whole(*moves[2]).wait_recv()
    with scope("finish0"):
        finish()
    with scope("back1"):
        whole(*moves[3]).wait_recv()
    with scope("leave"):
        for move in moves:
            whole(*move).wait_send()


def closing(
    sigma_half, dressed_half, green, last, sigma_hbm, dressed_hbm, wide, sigma, dressed, copy_sem
):
    def copy(source, target, part, lane):
        return pltpu.make_async_copy(source, target.at[pl.ds(part, source.shape[0])], copy_sem.at[lane])

    copies = [copy(sigma_half, sigma_hbm, 0, 0), copy(dressed_half, dressed_hbm, 0, 1)]
    for c in copies:
        c.start()
    for i in range(8):
        for side in range(2):
            rows = last[pl.ds(i * 32, 32), :, pl.ds(side * 128, 128)].astype(jnp.float32)
            wide[side, pl.ds(i * 256, 256), :] = rows.reshape(256, 128)

    def take(j):
        for side in range(2):
            rows = wide[side, pl.ds(j, 256, stride=8), :]
            sigma[j, :, pl.ds(side * 128, 128)] = rows.astype(jnp.bfloat16)

    reals = (0, 1, 4, 5)
    take(0)
    take(2)
    for n, real in enumerate(reals):
        if n < 3:
            take(reals[n + 1])
            take(reals[n + 1] + 2)
        dress(green.at[pl.ds(8, 8)], sigma, dressed, real)
        for part in (real, real + 2):
            copies.append(copy(dressed.at[pl.ds(part, 1)], dressed_hbm, 8 + part, 3 + part))
            copies[-1].start()
        if n == 2:
            copies.append(copy(sigma, sigma_hbm, 8, 2))
            copies[-1].start()
    with jax.named_scope("drain"):
        for c in copies:
            c.wait()


def per_device(green, screened):
    vmem = pl.BlockSpec(memory_space=pltpu.VMEM)
    hbm = pl.BlockSpec(memory_space=pltpu.HBM)
    blocks = pltpu.VMEM((HALVES, 256, 8, 256), jnp.bfloat16)
    half = jax.ShapeDtypeStruct((8, 256, 256), jnp.bfloat16)
    matrices = jax.ShapeDtypeStruct((16, 256, 256), jnp.bfloat16)
    wide = pltpu.VMEM((2, 2048, 128), jnp.float32)
    parts = pl.pallas_call(
        kernel,
        out_shape=(half, half, matrices, jax.ShapeDtypeStruct((256, 8, 256), jnp.bfloat16)),
        in_specs=[hbm] * 2,
        out_specs=[vmem] * 4,
        scratch_shapes=[
            pltpu.VMEM((2, 512, 128), jnp.float32),
            pltpu.VMEM((2, 1024, 128), jnp.float32),
            wide,
            blocks,
            blocks,
            blocks,
            pltpu.VMEM((256, 8, 256), jnp.bfloat16),
            pltpu.VMEM((1024, 1024), jnp.bfloat16),
            pltpu.VMEM((1024, 1024), jnp.bfloat16),
            pltpu.VMEM((1024, 512), jnp.bfloat16),
            pltpu.VMEM((1024, 512), jnp.bfloat16),
            pltpu.SemaphoreType.DMA((4,)),
            pltpu.SemaphoreType.DMA((4,)),
            pltpu.SemaphoreType.DMA((4,)),
        ],
        compiler_params=pltpu.CompilerParams(
            collective_id=0, has_side_effects=True, vmem_limit_bytes=VMEM_LIMIT
        ),
    )(green.reshape(16, 256, 256), pltpu.with_memory_space_constraint(screened.reshape(512, 256), pltpu.HBM))
    sigma, dressed = pl.pallas_call(
        closing,
        out_shape=(matrices, matrices),
        in_specs=[vmem] * 4,
        out_specs=[hbm] * 2,
        scratch_shapes=[
            wide,
            pltpu.VMEM((8, 256, 256), jnp.bfloat16),
            pltpu.VMEM((8, 256, 256), jnp.bfloat16),
            pltpu.SemaphoreType.DMA((11,)),
        ],
        compiler_params=pltpu.CompilerParams(vmem_limit_bytes=16 * 2**20),
    )(*parts)
    return sigma.reshape(green.shape), dressed.reshape(green.shape)


def solution(mesh):
    spread = P(None, None, "krow", "kcol", None, None)
    return jax.shard_map(
        per_device,
        mesh=mesh,
        in_specs=(spread, P(None, None, ("krow", "kcol"))),
        out_specs=(spread, spread),
        check_vma=False,
    )
```
